32 devices in a mesh: row: 4 (over x, core), col: 8 (over z, y).
Axes of the slice: x: 2, y: 2, z: 4, core: 2. Of those that a mesh axis runs over, the one named last changes fastest.
Arguments:
- ancestor_inv: bfloat16 [32, 32, 256, 256], P('row', 'col'), may hold values from -0.29882812 to 0.29882812
- lower_panel: bfloat16 [8, 16, 256, 256], P('row', 'col'), may hold values from -0.59765625 to 0.59765625
- upper_panel: bfloat16 [8, 16, 256, 256], P('col', 'row'), may hold values from -0.59765625 to 0.59765625
- pivot_inv: float32 [8, 256, 256], P('col'), may hold values from -6 to 6
- members: int32 [8, 16], replicated, may hold values from -1 to 31, as said below
Outputs:
- lower_inv: bfloat16 [8, 16, 256, 256], P('col', 'row')
- upper_inv: bfloat16 [8, 16, 256, 256], P('row', 'col')
- diag_inv: float32 [8, 256, 256], P('col')
The draws below stay inside these ranges and needn't reach their ends.
Inputs may be any that keep to these rules, and one draw needn't show every extreme that they name: `members`: slot s belongs to group g = s // 2; a used slot names an ancestor block of that group, from g * 4 to (g + 1) * 4 - 1. In each group of each supernode the used slots come first, name distinct blocks, and number 1 to 2; every group has 2 used slots for some supernode. Empty slots hold -1.
All inputs are finite; a program needn't handle non-finite values.
Results may differ from the reference program's by a relative error of at most 0.013.
Values may be sent and summed in bfloat16 or wider, within the bound.
No kernel may reach another device: no remote copies, remote signals or barrier semaphores. Data moves between devices by JAX's collectives and lax.ppermute only.
A program may use at most 128 MiB of HBM per device.

```python
from functools import partial
import jax
import jax.numpy as jnp
from jax import lax

B = 256
NBC = 4
CAP = 2
KL = 8
NB = 32
SLOTS = 16


def draw_members(key, part):
    groups = SLOTS // CAP
    key_counts, key_fullrow, key_ranking = jax.random.split(key, 3)
    counts = jax.random.randint(key_counts, (KL, groups), 1, CAP + 1)
    full_row = jax.random.randint(key_fullrow, (groups,), 0, KL)
    counts = jnp.where(jnp.arange(KL)[:, None] == full_row[None, :], CAP, counts)
    scores = jax.random.randint(key_ranking, (KL, groups, NBC), 0, 1 << 20) * NBC + jnp.arange(NBC)[None, None, :]
    ranking = jnp.argsort(scores, axis=-1)[:, :, :CAP]
    blocks = ranking + (jnp.arange(groups) * NBC)[None, :, None]
    in_use = jnp.arange(CAP)[None, None, :] < counts[:, :, None]
    return jnp.where(in_use, blocks, -1).astype(jnp.int32).reshape(KL, SLOTS)


def steps_of(own_key, dims, pieces, least, largest):
    loudness = 1.0
    for dim, parts in pieces:
        heights = jax.random.uniform(jax.random.fold_in(jax.random.fold_in(own_key, 6), dim), (parts,), jnp.float32, least / len(pieces), largest / len(pieces))
        loudness = loudness * jnp.repeat(jnp.exp(heights), dims[dim] // parts).reshape((-1,) + (1,) * (len(dims) - 1 - dim))
    return loudness


def gaussian(stream_key, shape, spread, reach, shards=(), dtype=jnp.bfloat16):
    entries = spread * jax.random.normal(stream_key, shape, jnp.float32)
    if shards:
        entries = entries * steps_of(stream_key, shape, shards, -0.22, 0.18)
    return jnp.clip(entries, -reach, reach).astype(dtype)


def setup_inputs(seed: int = 0) -> dict:
    streams_of = jax.random.split(jax.random.key(seed), 6)
    return {
        "ancestor_inv": gaussian(streams_of[0], (NB, NB, B, B), 0.05, 0.29882812, ((0, 4), (1, 8))),
        "lower_panel": gaussian(streams_of[1], (KL, SLOTS, B, B), 0.1, 0.59765625, ((0, 4), (1, 8))),
        "upper_panel": gaussian(streams_of[2], (KL, SLOTS, B, B), 0.1, 0.59765625, ((0, 8), (1, 4))),
        "pivot_inv": gaussian(streams_of[3], (KL, B, B), 1.0, 6.0, ((0, 8),), jnp.float32),
        "members": draw_members(jax.random.fold_in(streams_of[5], 71), 0),
    }


def one_supernode(ancestor_inv, item):
    member_row, lower_blocks, upper_blocks, pivot_block = item
    valid = member_row >= 0
    chosen = jnp.where(valid, member_row, 0).astype(jnp.int32)
    strip = jnp.take(ancestor_inv, chosen, axis=0)
    square = jnp.take(strip, chosen, axis=1).astype(jnp.float32)
    weight = valid.astype(jnp.float32)[:, None, None]
    lower_masked = lower_blocks.astype(jnp.float32) * weight
    upper_masked = upper_blocks.astype(jnp.float32) * weight
    lower_sum = -jnp.einsum("ijab,jbc->iac", square, lower_masked) * weight
    lower_inv = lower_sum.astype(jnp.bfloat16)
    upper_sum = -jnp.einsum("iab,ijbc->jac", upper_masked, square) * weight
    upper_inv = upper_sum.astype(jnp.bfloat16)
    diag_inv = pivot_block - jnp.einsum("iab,ibc->ac", upper_masked, lower_inv.astype(jnp.float32))
    return lower_inv, upper_inv, diag_inv


def reference(ancestor_inv, lower_panel, upper_panel, pivot_inv, members):
    lower_inv, upper_inv, diag_inv = lax.map(partial(one_supernode, ancestor_inv), (members, lower_panel, upper_panel, pivot_inv))
    return (lower_inv, upper_inv, diag_inv)
```

```python
from functools import partial
import jax
import jax.numpy as jnp
from jax import lax
from jax.experimental import pallas as pl
from jax.experimental.pallas import tpu as pltpu
from jax.sharding import PartitionSpec as P


def split(n):
    minor = max(d for d in range(1, n + 1) if n % d == 0 and d * d <= n)
    return n // minor, minor


class Line:
    def __init__(self, axis, n, other, major):
        self.axis, self.n, self.other, self.major = axis, n, other, major
        index = lax.axis_index(axis)
        self.pos = index // other if major else index % n

    def send(self, value, pairs):
        full = []
        for a, b in pairs:
            for q in range(self.other):
                if self.major:
                    full.append((a * self.other + q, b * self.other + q))
                else:
                    full.append((q * self.n + a, q * self.n + b))
        return lax.ppermute(value, self.axis, full)


def add(*terms):
    total = terms[0].astype(jnp.float32)
    for term in terms[1:]:
        total = total + term.astype(jnp.float32)
    return total


def gather_line(line, value):
    n = line.n
    if n == 1:
        return [(value, None)]
    if n == 2:
        return [(value, None), (line.send(value, [(0, 1), (1, 0)]), None)]
    right, left = [value], [value]
    for r in range(1, n):
        left.append(line.send(left[-1], [(p, p - 1) for p in range(1, n - r + 1)]))
        right.append(line.send(right[-1], [(p, p + 1) for p in range(r - 1, n - 1)]))
    return [(value, None)] + [(left[o], right[n - o]) for o in range(1, n)]


def pick(line, o, pair):
    return pair[0] if pair[1] is None else jnp.where(line.pos + o < line.n, pair[0], pair[1])


def slot_offset(pos, n, e):
    return jnp.where(pos < (n + 1) // 2, (n - e) % n, e)


def scatter_line(line, slots):
    n = line.n
    if n == 1:
        return add(slots[0])
    if n == 2:
        return add(slots[0], line.send(slots[1], [(0, 1), (1, 0)]))
    low = (n + 1) // 2
    near = line.pos < low
    from_left = from_right = None
    for t in range(1, n):
        senders = range(0, t)
        own = slots[t] if t <= low else jnp.where(near, slots[t], slots[n - t])
        out = own if from_left is None else add(own, from_left).astype(own.dtype)
        arrived_left = line.send(out, [(p, p + 1) for p in senders])
        senders = range(n - t, n)
        own = slots[t] if n - t >= low else jnp.where(near, slots[n - t], slots[t])
        out = own if from_right is None else add(own, from_right).astype(own.dtype)
        from_right = line.send(out, [(p, p - 1) for p in senders])
        from_left = arrived_left
    return add(slots[0], from_left, from_right)


def lower_kernel(dims, members, a_ref, *refs):
    (nx, nc, nz, ny, per_row, per_col, row_slots, cap, nrb, ncb) = dims
    pieces, outs = refs[: nx * nc], refs[nx * nc :]
    row, col = lax.axis_index("row"), lax.axis_index("col")
    x, c, z, y = row // nc, row % nc, col // ny, col % ny
    n_row = nx * nc

    def one(k, piece, q, out, at):
        lows = []
        for j in range(cap):
            m = members[k, col * cap + j]
            block = piece[q, j]
            lows.append((jnp.clip(m - col * ncb, 0, ncb - 1), jnp.where(m >= 0, block, jnp.zeros_like(block))))
        for i in range(row_slots):
            m = members[k, row * row_slots + i]
            r = jnp.clip(m - row * nrb, 0, nrb - 1)
            total = None
            for cj, block in lows:
                term = jnp.dot(a_ref[r, cj], block, preferred_element_type=jnp.float32)
                total = term if total is None else total + term
            out[at, i] = jnp.where(m >= 0, -total, 0.0).astype(out.dtype)

    for e in range(nz):
        for oy in range(ny):
            target = (z + slot_offset(z, nz, e)) % nz * ny + (y + slot_offset(y, ny, oy)) % ny
            for q in range(per_col):
                k = target * per_col + q
                source = k // per_row
                ox = (source // nc - x) % nx
                oc = (source % nc - c) % nc
                which = ox * nc + oc
                for w in range(n_row):

                    @pl.when(which == w)
                    def _(w=w):
                        one(k, pieces[w], k % per_row, outs[e * ny + oy], q)


def upper_kernel(dims, members, a_ref, *refs):
    (nx, nc, nz, ny, per_row, per_col, row_slots, cap, nrb, ncb) = dims
    n_pieces = sum(1 if oz == 0 else 2 for oz in range(nz)) * ny
    pieces, outs = refs[:n_pieces], refs[n_pieces:-2]
    u_ref, sem = refs[-2:]
    row, col = lax.axis_index("row"), lax.axis_index("col")
    x, c, z, y = row // nc, row % nc, col // ny, col % ny

    it = iter(pieces)
    copies = []
    for oy in range(ny):
        for oz in range(nz):
            column = (z + oz) % nz * ny + (y + oy) % ny
            copies.append((column, oz, [next(it)] if oz == 0 else [next(it), next(it)]))
    for n, (column, oz, sources) in enumerate(copies):
        for s, source in enumerate(sources):
            take = True if len(sources) == 1 else (z + oz < nz if s == 0 else z + oz >= nz)

            def start(source=source, column=column, n=n):
                pltpu.make_async_copy(source, u_ref.at[column], sem.at[n]).start()

            if take is True:
                start()
            else:
                pl.when(take)(start)
    for n, (column, oz, sources) in enumerate(copies):
        pltpu.make_async_copy(sources[0], u_ref.at[column], sem.at[n]).wait()

    for oc in range(nc):
        for ox in range(nx):
            target = (x + ox) % nx * nc + (c + oc) % nc
            for q in range(per_row):
                k = target * per_row + q
                blocks = []
                for i in range(row_slots):
                    m = members[k, row * row_slots + i]
                    block = u_ref[k // per_col, k % per_col, i]
                    blocks.append((jnp.clip(m - row * nrb, 0, nrb - 1), jnp.where(m >= 0, block, jnp.zeros_like(block))))
                for j in range(cap):
                    m = members[k, col * cap + j]
                    cj = jnp.clip(m - col * ncb, 0, ncb - 1)
                    total = None
                    for r, block in blocks:
                        term = jnp.dot(block, a_ref[r, cj], preferred_element_type=jnp.float32)
                        total = term if total is None else total + term
                    outs[oc * nx + ox][q, j] = jnp.where(m >= 0, -total, 0.0).astype(jnp.bfloat16)


def body(ancestor_inv, lower_panel, upper_panel, pivot_inv, members):
    n_col, n_row = lax.axis_size("col"), lax.axis_size("row")
    row, col = lax.axis_index("row"), lax.axis_index("col")
    nrb, ncb, side, _ = ancestor_inv.shape
    per_row, cap = lower_panel.shape[:2]
    per_col, row_slots = upper_panel.shape[:2]
    nz, ny = split(n_col)
    nx, nc = split(n_row)
    zline, yline = Line("col", nz, ny, True), Line("col", ny, nz, False)
    xline, cline = Line("row", nx, nc, True), Line("row", nc, nx, False)
    dims = (nx, nc, nz, ny, per_row, per_col, row_slots, cap, nrb, ncb)
    smem = pl.BlockSpec(memory_space=pltpu.SMEM)
    vmem = pl.BlockSpec(memory_space=pltpu.VMEM)
    hbm = pl.BlockSpec(memory_space=pltpu.MemorySpace.HBM)
    half = jnp.bfloat16

    pieces = []
    for ox, pair in enumerate(gather_line(xline, lower_panel)):
        for oc, inner in enumerate(gather_line(cline, pick(xline, ox, pair))):
            pieces.append(pick(cline, oc, inner))
    part = jax.ShapeDtypeStruct((per_col, row_slots, side, side), half)
    lower_parts = pl.pallas_call(
        partial(lower_kernel, dims),
        out_shape=[part] * n_col,
        in_specs=[smem, vmem] + [vmem] * n_row,
        out_specs=[vmem] * n_col,
    )(members, ancestor_inv, *pieces)

    uppers = []
    for oy, pair in enumerate(gather_line(yline, upper_panel)):
        for inner in gather_line(zline, pick(yline, oy, pair)):
            uppers.extend(v for v in inner if v is not None)
    share = jax.ShapeDtypeStruct((per_row, cap, side, side), half)
    upper_parts = pl.pallas_call(
        partial(upper_kernel, dims),
        out_shape=[share] * n_row,
        in_specs=[smem, vmem] + [hbm] * len(uppers),
        out_specs=[vmem] * n_row,
        scratch_shapes=[
            pltpu.VMEM((n_col, per_col, row_slots, side, side), half),
            pltpu.SemaphoreType.DMA((n_col,)),
        ],
    )(members, ancestor_inv, *uppers)

    slots = []
    for e in range(nz):
        slots.append(scatter_line(yline, lower_parts[e * ny : (e + 1) * ny]).astype(half))
    lower_inv = scatter_line(zline, slots).astype(half)

    slots = [None] * nx
    for e in range(nx):
        pass
    by_core = [upper_parts[oc * nx : (oc + 1) * nx] for oc in range(nc)]
    sums = [scatter_line(cline, [by_core[oc][ox] for oc in range(nc)]).astype(half) for ox in range(nx)]
    if nx > 2:
        order = [slot_offset(xline.pos, nx, e) for e in range(nx)]
        stacked = jnp.stack(sums)
        sums = [lax.dynamic_index_in_dim(stacked, o, 0, keepdims=False) for o in order]
    upper_inv = scatter_line(xline, sums).astype(half)

    own = lax.dynamic_slice(members, (col * per_col, row * row_slots), (per_col, row_slots)) >= 0
    own_upper = jnp.where(own[:, :, None, None], upper_panel, jnp.zeros((), half))
    diag = jnp.einsum("kiab,kibc->kac", own_upper, lower_inv, preferred_element_type=jnp.float32)
    diag = scatter_all(cline, diag)
    diag = scatter_all(xline, lax.reduce_precision(diag, 8, 7).astype(half))
    return lower_inv, upper_inv, pivot_inv - diag


def scatter_all(line, value):
    terms = [pick(line, o, pair) for o, pair in enumerate(gather_line(line, value))]
    if line.n > 2:
        stacked = jnp.stack(terms)
        terms = [lax.dynamic_index_in_dim(stacked, (p - line.pos) % line.n, 0, keepdims=False) for p in range(line.n)]
    return add(*terms)


def solution(mesh):
    return jax.shard_map(
        body,
        mesh=mesh,
        in_specs=(
            P("row", "col", None, None),
            P("row", "col", None, None),
            P("col", "row", None, None),
            P("col", None, None),
            P(),
        ),
        out_specs=(P("col", "row", None, None), P("row", "col", None, None), P("col", None, None)),
        check_vma=False,
    )
```
